32 devices in a mesh: rows: 8 (over z, x), cols: 4 (over y, core).
Axes of the slice: x: 2, y: 2, z: 4, core: 2. Of those that a mesh axis runs over, the one named last changes fastest.
Arguments:
- kernel_hat: bfloat16 [2, 256, 512, 1024], P(None, 'rows', 'cols'), may hold values from -0.5 to 0.5
- coefficients: float32 [128, 512], P(None, 'cols'), may hold values from -6 to 6
- wave_speed_sq: float32 [2048, 1024], P('rows', 'cols'), may hold values from 1 to 4
- wet_mask: int32 [2048, 1024], P('rows', 'cols'), may hold values 0 or 1
- boundary_cell: int32 [1024], replicated, may hold values from 0 to 1023, each once
- height: float32 [2048, 1024], P('rows', 'cols'), may hold values from -3 to 3
- flux_x: float32 [2048, 1024], P('rows', 'cols'), may hold values from -3 to 3
- flux_y: float32 [2048, 1024], P('rows', 'cols'), may hold values from -3 to 3
Outputs:
- boundary_series: float32 [128, 1024], P('rows', 'cols')
- height_out: float32 [2048, 1024], P('rows', 'cols')
- flux_x_out: float32 [2048, 1024], P('rows', 'cols')
- flux_y_out: float32 [2048, 1024], P('rows', 'cols')
The draws below stay inside these ranges and needn't reach their ends.
Inputs may be any that keep to these rules, and one draw needn't show every extreme that they name: `boundary_cell`: each of the 1024 boundary points names a different grid column, so each column is named by exactly one point.
All inputs are finite; a program needn't handle non-finite values. No bound on the sum of `wet_mask` on one device may be relied on, other than what follows from the above.
Results may differ from the reference program's by a relative error of at most 0.0029.
Values sent between devices are 32-bit elements; how exact they have to be, the bound alone decides.
A program may use at most 64 MiB of HBM per device.

```python
import math
import jax
import jax.numpy as jnp
from jax import lax

NT = 128
SRC = 512
NF = 256
OBS = 1024
NR = 2048
NC = 1024


def touch_ends(array, own_key, least, top_value):
    longest = array.shape.index(max(array.shape))
    spots = []
    for shift in (0, 1):
        where = [jax.random.randint(jax.random.fold_in(own_key, axis), (), 0, length) for axis, length in enumerate(array.shape)]
        where[longest] = (where[longest] + shift) % array.shape[longest]
        spots.append(tuple(where))
    return array.at[spots[0]].set(least).at[spots[1]].set(top_value)


def block_scale(rng, extent, shards, least, largest):
    factor_of, own = 1.0, jax.random.fold_in(rng, 6)
    for axis_at, shards_of in shards:
        steps = jnp.exp(jax.random.uniform(jax.random.fold_in(own, axis_at), (shards_of,), jnp.float32, least / len(shards), largest / len(shards)))
        factor_of = factor_of * jnp.repeat(steps, extent[axis_at] // shards_of).reshape([-1 if axis == axis_at else 1 for axis in range(len(extent))])
    return factor_of


def scatter_about(key, shape, width, reach, cuts=(), kind=jnp.bfloat16):
    values = width * jax.random.normal(key, shape, jnp.float32)
    if cuts:
        values = values * block_scale(key, shape, cuts, -0.22, 0.18)
    return jnp.clip(values, -reach, reach).astype(kind)


def setup_inputs(seed: int = 0) -> dict:
    keys = jax.random.split(jax.random.key(seed), 9)
    return {
        "kernel_hat": scatter_about(keys[0], (2, NF, SRC, OBS), (SRC // 4) ** -0.5, 0.5, ((1, 8), (2, 4))),
        "coefficients": scatter_about(keys[1], (NT, SRC), 1.0, 6.0, ((1, 4),), jnp.float32),
        "wave_speed_sq": jnp.clip(jnp.exp(math.log(4.0) - 1.3862944 * jax.random.uniform(keys[2], (NR, NC), jnp.float32) ** block_scale(keys[2], (NR, NC), ((0, 8), (1, 4)), -0.2, 0.2)), 1.0, 4.0),
        "wet_mask": touch_ends((jax.random.randint(keys[3], (NR, NC), 0, 4) < 3).astype(jnp.int32), jax.random.fold_in(keys[3], 1), 0, 1),
        "boundary_cell": jax.random.permutation(keys[4], OBS).astype(jnp.int32),
        "height": scatter_about(keys[5], (NR, NC), 0.5, 3.0, ((0, 8), (1, 4)), jnp.float32),
        "flux_x": scatter_about(keys[6], (NR, NC), 0.5, 3.0, ((0, 8), (1, 4)), jnp.float32),
        "flux_y": scatter_about(keys[7], (NR, NC), 0.5, 3.0, ((0, 8), (1, 4)), jnp.float32),
    }


STEP_RATIO = 0.25

def neighbours(values, along_dim):
    if along_dim == 1:
        return (values[1:-1, :-1], values[1:-1, 1:])
    return (values[:-1, 1:-1], values[1:, 1:-1])

def face_fluxes(surface, along, across, speed_sq, celerity, wet, along_dim):
    left_surf, right_surf = neighbours(surface, along_dim)
    left_along, right_along = neighbours(along, along_dim)
    left_across, right_across = neighbours(across, along_dim)
    left_sq, right_sq = neighbours(speed_sq, along_dim)
    left_speed, right_speed = neighbours(celerity, along_dim)
    left_wet, right_wet = neighbours(wet, along_dim)
    opened = left_wet * right_wet
    damping = 0.25 * (left_speed + right_speed)
    mass_flux = opened * (0.5 * (left_along + right_along) - damping * (right_surf - left_surf))
    momentum = opened * (0.5 * (left_sq * left_surf + right_sq * right_surf) - damping * (right_along - left_along))
    shear_flux = opened * (-damping * (right_across - left_across))
    return (mass_flux, momentum, shear_flux)

def advance(surface, along_x, along_y, speed_sq, wet):
    celerity = jnp.sqrt(speed_sq)
    mass_x, momentum_x, shear_x = face_fluxes(surface, along_x, along_y, speed_sq, celerity, wet, 1)
    mass_y, momentum_y, shear_y = face_fluxes(surface, along_y, along_x, speed_sq, celerity, wet, 0)
    interior_wet = wet[1:-1, 1:-1]

    def update(values, flux_cols, flux_rows):
        change = flux_cols[:, 1:] - flux_cols[:, :-1] + (flux_rows[1:] - flux_rows[:-1])
        return interior_wet * (values[1:-1, 1:-1] - STEP_RATIO * change)
    return (update(surface, mass_x, mass_y), update(along_x, momentum_x, shear_y), update(along_y, shear_x, momentum_y))

def reference(kernel_hat, coefficients, wave_speed_sq, wet_mask, boundary_cell, height, flux_x, flux_y):
    spectrum = jnp.fft.fft(coefficients, n=NF, axis=0)
    coef_re = lax.optimization_barrier(jnp.real(spectrum).astype(jnp.bfloat16)).astype(jnp.float32)
    coef_im = lax.optimization_barrier(jnp.imag(spectrum).astype(jnp.bfloat16)).astype(jnp.float32)
    high = lax.Precision.HIGHEST

    def one_frequency(index):
        kern_re = lax.dynamic_index_in_dim(kernel_hat[0], index, 0, keepdims=False).astype(jnp.float32)
        kern_im = lax.dynamic_index_in_dim(kernel_hat[1], index, 0, keepdims=False).astype(jnp.float32)
        row_re = lax.dynamic_index_in_dim(coef_re, index, 0, keepdims=False)
        row_im = lax.dynamic_index_in_dim(coef_im, index, 0, keepdims=False)
        spec_re = jnp.dot(row_re, kern_re, precision=high) - jnp.dot(row_im, kern_im, precision=high)
        spec_im = jnp.dot(row_im, kern_re, precision=high) + jnp.dot(row_re, kern_im, precision=high)
        return (spec_re, spec_im)
    spec_re, spec_im = lax.map(one_frequency, jnp.arange(NF, dtype=jnp.int32))
    times = jnp.arange(NT, dtype=jnp.int32)
    freqs = jnp.arange(NF, dtype=jnp.int32)
    phase = (times[:, None] * freqs[None, :] % NF).astype(jnp.float32) * (2.0 * math.pi / NF)
    series = (jnp.dot(jnp.cos(phase), spec_re, precision=high) - jnp.dot(jnp.sin(phase), spec_im, precision=high)) / NF
    latest = series[NT - 2:]
    ghost = jnp.zeros((2, NC), jnp.float32).at[:, boundary_cell].set(latest)
    wet = wet_mask.astype(jnp.float32)
    speed_pad = jnp.pad(wave_speed_sq, 1).at[-1].set(1.0)
    wet_pad = jnp.pad(wet, 1).at[-1].set(1.0)
    surface, along_x, along_y = (height, flux_x, flux_y)
    for step in range(2):
        surf_pad = jnp.pad(surface, 1).at[-1, 1:-1].set(ghost[step])
        surface, along_x, along_y = advance(surf_pad, jnp.pad(along_x, 1), jnp.pad(along_y, 1), speed_pad, wet_pad)
    return (series, surface, along_x, along_y)
```

```python
import functools
import math

import jax
import jax.numpy as jnp
import numpy as np
from jax import lax
from jax.experimental import pallas as pl
from jax.experimental.pallas import tpu as pltpu
from jax.sharding import PartitionSpec as P

MESH = pl.DeviceIdType.MESH
GROUP = 8
EDGE = 8
LANE = 128
F32 = jnp.float32
BF16 = jnp.bfloat16


def tables(freq_total, steps, row_devs):
    freq = np.arange(freq_total)
    time = np.arange(steps)
    phase = 2.0 * math.pi * (np.outer(freq, time) % freq_total) / freq_total
    cos = np.cos(phase).reshape(row_devs, -1, GROUP, steps)
    sin = np.sin(phase).reshape(row_devs, -1, GROUP, steps)
    both = np.concatenate([cos, -sin], axis=2).reshape(row_devs, -1, steps)
    forward = both.astype(np.float32)
    inverse = np.swapaxes(both, 1, 2) / freq_total
    high = inverse.astype(np.float32).astype(jnp.bfloat16)
    low = (inverse - high.astype(np.float64)).astype(np.float32).astype(jnp.bfloat16)
    return forward, np.concatenate([high, high, low], axis=2)


def split(value):
    high = value.astype(BF16)
    return high, value - high.astype(F32)


def faces(speed, wet, dim):
    ahead = speed.shape[dim] - 1
    opened = wet * pltpu.roll(wet, ahead, dim)
    return 0.5 * opened, opened * (0.25 * (speed + pltpu.roll(speed, ahead, dim)))


def step_once(surf, qx, qy, speed_sq, wet, face_x, face_y):
    energy = speed_sq * surf
    change = []
    for dim, along, across, (half, damp) in ((1, qx, qy, face_x), (0, qy, qx, face_y)):
        ahead = surf.shape[dim] - 1
        later = lambda v: pltpu.roll(v, ahead, dim)
        mass = half * (along + later(along)) - damp * (later(surf) - surf)
        momentum = half * (energy + later(energy)) - damp * (later(along) - along)
        shear = -damp * (later(across) - across)
        change.append([f - pltpu.roll(f, 1, dim) for f in (mass, momentum, shear)])
    (mass_x, mom_x, shear_x), (mass_y, mom_y, shear_y) = change
    return (
        wet * (surf - 0.25 * (mass_x + mass_y)),
        wet * (qx - 0.25 * (mom_x + shear_y)),
        wet * (qy - 0.25 * (shear_x + mom_y)),
    )


def kernel(
    n_rows, n_cols,
    kern_hbm, coef_hbm, sq_hbm, wet_hbm, cell_hbm, surf_hbm, qx_hbm, qy_hbm, fwd_hbm, inv_hbm,
    series_hbm, surf_out, qx_out, qy_out,
    kern, coef, fwd, inv, cells, pad, wet_int, wet_pad, corner, corner_wet,
    strip_out, strip_in, spec_out, spec_in, whole_buf, whole_in, series_buf, late_in,
    mid, out_buf,
    local_sem, kern_sem, halo_send, halo_recv, spec_send, spec_recv,
    whole_send, whole_recv, late_send, late_recv, out_sem,
):
    row = lax.axis_index("rows")
    col = lax.axis_index("cols")
    freqs, src, obs = kern.shape[1:]
    groups = freqs // GROUP
    tall, wide = surf_hbm.shape
    points = obs // n_cols
    own_steps = series_buf.shape[0]
    has_n, has_s = row > 0, row < n_rows - 1
    has_w, has_e = col > 0, col < n_cols - 1
    at_edge = row == n_rows - 1

    inputs = [
        pltpu.make_async_copy(coef_hbm, coef, local_sem.at[0]),
        pltpu.make_async_copy(fwd_hbm.at[row], fwd, local_sem.at[1]),
        pltpu.make_async_copy(surf_hbm, pad.at[0, :tall, :wide], local_sem.at[2]),
        pltpu.make_async_copy(qx_hbm, pad.at[1, :tall, :wide], local_sem.at[3]),
        pltpu.make_async_copy(qy_hbm, pad.at[2, :tall, :wide], local_sem.at[4]),
        pltpu.make_async_copy(sq_hbm, pad.at[3, :tall, :wide], local_sem.at[5]),
        pltpu.make_async_copy(wet_hbm, wet_int.at[:tall], local_sem.at[6]),
        pltpu.make_async_copy(inv_hbm.at[row], inv, local_sem.at[7]),
        pltpu.make_async_copy(cell_hbm, cells, local_sem.at[8]),
    ]
    for copy in inputs:
        copy.start()
    chunks = []
    for g in range(groups):
        for part in range(2):
            where = pl.ds(g * GROUP, GROUP)
            copy = pltpu.make_async_copy(
                kern_hbm.at[part, where], kern.at[part, where], kern_sem.at[g, part]
            )
            copy.start()
            chunks.append(copy)

    diagonals = [
        (has_n & has_w, -1, -1), (has_n & has_e, -1, 1),
        (has_s & has_w, 1, -1), (has_s & has_e, 1, 1),
    ]
    barrier = pltpu.get_barrier_semaphore()
    for k in range(1, n_rows):
        pl.semaphore_signal(barrier, 1, device_id=(lax.rem(row + k, n_rows), col), device_id_type=MESH)
    for k in range(1, n_cols):
        pl.semaphore_signal(barrier, 1, device_id=(row, lax.rem(col + k, n_cols)), device_id_type=MESH)
    for exists, dr, dc in diagonals:
        @pl.when(exists)
        def _(dr=dr, dc=dc):
            pl.semaphore_signal(barrier, 1, device_id=(row + dr, col + dc), device_id_type=MESH)

    inputs[0].wait()
    inputs[1].wait()
    spectrum = jnp.dot(
        fwd[...], coef[...], precision=lax.Precision.HIGHEST, preferred_element_type=F32
    )

    for copy in inputs[2:7]:
        copy.wait()
    lane = lax.broadcasted_iota(jnp.int32, (tall, LANE), 1)
    packed = jnp.zeros((tall, LANE), F32)
    for k in range(5):
        if k < 4:
            first, last = pad[k, :tall, :LANE], pad[k, :tall, wide - LANE:wide]
        else:
            first = wet_int[:tall, :LANE].astype(F32)
            last = wet_int[:tall, wide - LANE:wide].astype(F32)
        at = 2 * k
        moved = first if at == 0 else pltpu.roll(first, at, 1)
        packed = jnp.where((lane >= at) & (lane < at + 2), moved, packed)
        at = 16 + 2 * k
        packed = jnp.where(
            (lane >= at) & (lane < at + 2), pltpu.roll(last, at + 2, 1), packed
        )
    strip_out[...] = packed.T[:32]

    pl.semaphore_wait(
        barrier,
        n_rows - 1 + n_cols - 1 + sum(exists.astype(jnp.int32) for exists, _, _ in diagonals),
    )

    def remote(source, target, sems, index, to):
        return pltpu.make_async_remote_copy(
            src_ref=source, dst_ref=target, send_sem=sems[0].at[index], recv_sem=sems[1].at[index],
            device_id=to, device_id_type=MESH,
        )

    halo = (halo_send, halo_recv)
    north = (lax.rem(row + n_rows - 1, n_rows), col)
    south = (lax.rem(row + 1, n_rows), col)
    west = (row, lax.rem(col + n_cols - 1, n_cols))
    east = (row, lax.rem(col + 1, n_cols))
    top, bottom = pl.ds(0, EDGE), pl.ds(tall - EDGE, EDGE)
    south_halo, north_halo = pl.ds(tall, EDGE), pl.ds(tall + EDGE, EDGE)
    body = pl.ds(0, wide)
    moves = [
        (has_n, has_s, [
            remote(pad.at[:, top, body], pad.at[:, south_halo, body], halo, 0, north),
            remote(wet_int.at[top], wet_int.at[south_halo], halo, 1, north)]),
        (has_s, has_n, [
            remote(pad.at[:, bottom, body], pad.at[:, north_halo, body], halo, 2, south),
            remote(wet_int.at[bottom], wet_int.at[north_halo], halo, 3, south)]),
        (has_w, has_e, [remote(strip_out.at[pl.ds(0, 16)], strip_in.at[pl.ds(16, 16)], halo, 4, west)]),
        (has_e, has_w, [remote(strip_out.at[pl.ds(16, 16)], strip_in.at[pl.ds(0, 16)], halo, 5, east)]),
    ]
    for i, (exists, dr, dc) in enumerate(diagonals):
        rows_at = top if dr < 0 else bottom
        cols_at = pl.ds(0, LANE) if dc < 0 else pl.ds(wide - LANE, LANE)
        to = (lax.rem(row + dr + n_rows, n_rows), lax.rem(col + dc + n_cols, n_cols))
        moves.append((exists, diagonals[3 - i][0], [
            remote(pad.at[:, rows_at, cols_at], corner.at[i], halo, 6 + 2 * i, to),
            remote(wet_int.at[rows_at, cols_at], corner_wet.at[i], halo, 7 + 2 * i, to)]))
    for exists, _, copies in moves:
        @pl.when(exists)
        def _(copies=copies):
            for copy in copies:
                copy.start()

    lanes16 = lax.broadcasted_iota(jnp.int32, (2 * GROUP, src), 0) % GROUP
    spec_copies = []
    for g in range(groups):
        mine = spectrum[g * 2 * GROUP:(g + 1) * 2 * GROUP]
        turned = jnp.concatenate([-mine[GROUP:], mine[:GROUP]], axis=0)
        total = None
        for part, value in enumerate((mine, turned)):
            chunks[2 * g + part].wait()
            value = value.astype(BF16).astype(F32)
            if src % LANE == 0:
                left = jnp.concatenate(
                    [jnp.where(lanes16 == j, value, 0.0) for j in range(GROUP)], axis=1
                ).astype(BF16)
                right = kern[part, pl.ds(g * GROUP, GROUP)].reshape(GROUP * src, obs)
                term = jnp.dot(left, right, preferred_element_type=F32)
                total = term if total is None else total + term
            else:
                for j in range(GROUP):
                    term = jnp.dot(
                        jnp.where(lanes16 == j, value, 0.0).astype(BF16),
                        kern[part, g * GROUP + j], preferred_element_type=F32,
                    )
                    total = term if total is None else total + term
        for d in range(n_cols):
            spec_out[d, g] = total[:, d * points:(d + 1) * points]
        for k in range(1, n_cols):
            to = lax.rem(col + k, n_cols)
            copy = remote(
                spec_out.at[to, g], spec_in.at[k - 1, g], (spec_send.at[g], spec_recv.at[g]),
                k - 1, (row, to),
            )
            copy.start()
            spec_copies.append(copy)

    for i, (_, arrives, copies) in enumerate(moves):
        @pl.when(arrives)
        def _(copies=copies):
            for copy in copies:
                copy.wait_recv()

        @pl.when(jnp.logical_not(arrives))
        def _(i=i):
            if i == 0:
                pad[:, south_halo, body] = jnp.zeros((4, EDGE, wide), F32)
                wet_int[south_halo] = jnp.zeros((EDGE, wide), jnp.int32)
            elif i == 1:
                pad[:, north_halo, body] = jnp.zeros((4, EDGE, wide), F32)
                wet_int[north_halo] = jnp.zeros((EDGE, wide), jnp.int32)
            elif i == 2:
                strip_in[pl.ds(16, 16)] = jnp.zeros((16, tall), F32)
            elif i == 3:
                strip_in[pl.ds(0, 16)] = jnp.zeros((16, tall), F32)
            else:
                corner[i - 4] = jnp.zeros((4, EDGE, LANE), F32)
                corner_wet[i - 4] = jnp.zeros((EDGE, LANE), jnp.int32)

    beside = jnp.concatenate([strip_in[...], jnp.zeros((LANE - 32, tall), F32)], axis=0).T
    wet_pad[:, :wide] = wet_int[...].astype(F32)
    near = lax.broadcasted_iota(jnp.int32, (EDGE, LANE), 1) < LANE // 2
    for k in range(5):
        side = jnp.where(
            lane < LANE // 2,
            pltpu.roll(beside, LANE - 16 - 2 * k, 1),
            pltpu.roll(beside, LANE - 2 - 2 * k, 1),
        )
        pick = (lambda i: corner[i, k]) if k < 4 else (lambda i: corner_wet[i].astype(F32))
        low = jnp.where(near, pick(0), pick(1))
        high = jnp.where(near, pick(2), pick(3))
        if k < 4:
            pad[k, :tall, wide:] = side
            pad[k, tall:tall + EDGE, wide:] = low
            pad[k, tall + EDGE:, wide:] = high
        else:
            wet_pad[:tall, wide:] = side
            wet_pad[tall:tall + EDGE, wide:] = low
            wet_pad[tall + EDGE:, wide:] = high

    @pl.when(at_edge)
    def _():
        pad[3, tall:tall + 1, :] = jnp.ones((1, wide + LANE), F32)
        wet_pad[tall:tall + 1, :] = jnp.ones((1, wide + LANE), F32)

    def first_step():
        wet, speed_sq = wet_pad[...], pad[3]
        speed = jnp.sqrt(speed_sq)
        face_x, face_y = faces(speed, wet, 1), faces(speed, wet, 0)
        new = step_once(pad[0], pad[1], pad[2], speed_sq, wet, face_x, face_y)
        for k in range(3):
            mid[k] = new[k]

    def second_step():
        wet, speed_sq = wet_pad[...], pad[3]
        speed = jnp.sqrt(speed_sq)
        face_x, face_y = faces(speed, wet, 1), faces(speed, wet, 0)
        new = step_once(mid[0], mid[1], mid[2], speed_sq, wet, face_x, face_y)
        for k in range(3):
            out_buf[k] = new[k][:tall, :wide]

    first_step()

    for copy in spec_copies:
        copy.wait_recv()
    highs, lows = [], []
    for g in range(groups):
        value = spec_out[col, g]
        for k in range(1, n_cols):
            value = value + spec_in[k - 1, g]
        high, low = split(value)
        highs.append(high)
        lows.append(low.astype(BF16))
    inputs[7].wait()
    whole_buf[...] = jnp.dot(
        inv[...], jnp.concatenate(highs + lows + highs, axis=0), preferred_element_type=F32
    )
    whole_copies = []
    for k in range(1, n_rows):
        to = lax.rem(row + k, n_rows)
        copy = remote(
            whole_buf.at[pl.ds(pl.multiple_of(to * own_steps, own_steps), own_steps)],
            whole_in.at[k - 1], (whole_send, whole_recv), k - 1, (to, col),
        )
        copy.start()
        whole_copies.append(copy)

    second_step()
    outs = (surf_out, qx_out, qy_out)
    results = []
    for k in range(3):
        where = pl.ds(0, tall - EDGE)
        results.append(pltpu.make_async_copy(out_buf.at[k, where], outs[k].at[where], out_sem.at[k]))
        results[-1].start()
    inputs[8].wait()

    for copy in whole_copies:
        copy.wait_recv()
    value = whole_buf[pl.ds(pl.multiple_of(row * own_steps, own_steps), own_steps)]
    for k in range(1, n_rows):
        value = value + whole_in[k - 1]
    series_buf[...] = value
    results.append(pltpu.make_async_copy(series_buf, series_hbm, out_sem.at[3]))
    results[-1].start()

    late_copies = [
        remote(
            series_buf.at[pl.ds(own_steps - EDGE, EDGE)], late_in.at[col], (late_send, late_recv),
            k - 1, (row, lax.rem(col + k, n_cols)),
        )
        for k in range(1, n_cols)
    ]

    @pl.when(at_edge)
    def _():
        for copy in late_copies:
            copy.start()
        span = wide + LANE
        place = lax.broadcasted_iota(jnp.int32, (span, obs), 0)
        place = jnp.where(place >= wide + LANE // 2, place - span, place) + col * wide
        chosen = jnp.where(place == cells[...], 1.0, 0.0).astype(BF16)
        late_in[col] = value[own_steps - EDGE:]
        for k in range(1, n_cols):
            come = lax.rem(col + n_cols - k, n_cols)
            remote(
                series_buf.at[pl.ds(own_steps - EDGE, EDGE)], late_in.at[come],
                (late_send, late_recv), k - 1, (row, lax.rem(col + k, n_cols)),
            ).wait_recv()
        latest = jnp.concatenate([late_in[d] for d in range(n_cols)], axis=1)
        high, rest = split(latest)
        middle, rest = split(rest)
        parts = jnp.concatenate([high.astype(F32), middle.astype(F32), rest, rest], axis=0)
        picked = lax.dot_general(
            parts.astype(BF16), chosen, (((1,), (1,)), ((), ())), preferred_element_type=F32
        )
        picked = picked[:EDGE] + picked[EDGE:2 * EDGE] + picked[2 * EDGE:3 * EDGE]
        base = tall - 2 * EDGE
        part_rows = pl.ds(base, 3 * EDGE)
        at_ghost = lax.broadcasted_iota(jnp.int32, (3 * EDGE, span), 0) == 2 * EDGE
        ghosts = [
            jnp.broadcast_to(picked[EDGE - 2 + k:EDGE - 1 + k], (3 * EDGE, span)) for k in range(2)
        ]
        wet, speed_sq = wet_pad[part_rows], pad[3, part_rows]
        speed = jnp.sqrt(speed_sq)
        face_x, face_y = faces(speed, wet, 1), faces(speed, wet, 0)
        surf = jnp.where(at_ghost, ghosts[0], pad[0, part_rows])
        surf, qx, qy = step_once(
            surf, pad[1, part_rows], pad[2, part_rows], speed_sq, wet, face_x, face_y
        )
        surf = jnp.where(at_ghost, ghosts[1], surf)
        qx = jnp.where(at_ghost, 0.0, qx)
        qy = jnp.where(at_ghost, 0.0, qy)
        new = step_once(surf, qx, qy, speed_sq, wet, face_x, face_y)
        for k in range(3):
            out_buf[k, tall - EDGE:] = new[k][EDGE:2 * EDGE, :wide]

    for k in range(3):
        where = pl.ds(tall - EDGE, EDGE)
        results.append(
            pltpu.make_async_copy(out_buf.at[k, where], outs[k].at[where], out_sem.at[4 + k])
        )
        results[-1].start()
    for exists, _, copies in moves:
        @pl.when(exists)
        def _(copies=copies):
            for copy in copies:
                copy.wait_send()
    for copy in spec_copies + whole_copies:
        copy.wait_send()

    @pl.when(at_edge)
    def _():
        for copy in late_copies:
            copy.wait_send()

    for copy in results:
        copy.wait()


def on_device(n_rows, n_cols, kernel_hat, coefficients, wave_speed_sq, wet_mask, boundary_cell, height, flux_x, flux_y):
    _, freqs, src, obs = kernel_hat.shape
    steps = coefficients.shape[0]
    tall, wide = height.shape
    groups = freqs // GROUP
    points = obs // n_cols
    own_steps = steps // n_rows
    span = wide + LANE
    forward, inverse = tables(freqs * n_rows, steps, n_rows)
    dma = pltpu.SemaphoreType.DMA
    anywhere = pl.BlockSpec(memory_space=pl.ANY)
    return pl.pallas_call(
        functools.partial(kernel, n_rows, n_cols),
        out_shape=(
            jax.ShapeDtypeStruct((own_steps, points), F32),
            jax.ShapeDtypeStruct((tall, wide), F32),
            jax.ShapeDtypeStruct((tall, wide), F32),
            jax.ShapeDtypeStruct((tall, wide), F32),
        ),
        in_specs=[anywhere] * 10,
        out_specs=(anywhere,) * 4,
        scratch_shapes=[
            pltpu.VMEM(kernel_hat.shape, BF16),
            pltpu.VMEM(coefficients.shape, F32),
            pltpu.VMEM(forward.shape[1:], F32),
            pltpu.VMEM(inverse.shape[1:], BF16),
            pltpu.VMEM((1, obs), jnp.int32),
            pltpu.VMEM((4, tall + 2 * EDGE, span), F32),
            pltpu.VMEM((tall + 2 * EDGE, wide), jnp.int32),
            pltpu.VMEM((tall + 2 * EDGE, span), F32),
            pltpu.VMEM((4, 4, EDGE, LANE), F32),
            pltpu.VMEM((4, EDGE, LANE), jnp.int32),
            pltpu.VMEM((32, tall), F32),
            pltpu.VMEM((32, tall), F32),
            pltpu.VMEM((n_cols, groups, 2 * GROUP, points), F32),
            pltpu.VMEM((n_cols - 1, groups, 2 * GROUP, points), F32),
            pltpu.VMEM((steps, points), F32),
            pltpu.VMEM((n_rows - 1, own_steps, points), F32),
            pltpu.VMEM((own_steps, points), F32),
            pltpu.VMEM((n_cols, EDGE, points), F32),
            pltpu.VMEM((3, tall + 2 * EDGE, span), F32),
            pltpu.VMEM((3, tall, wide), F32),
            dma((9,)),
            dma((groups, 2)),
            dma((14,)),
            dma((14,)),
            dma((groups, n_cols - 1)),
            dma((groups, n_cols - 1)),
            dma((n_rows - 1,)),
            dma((n_rows - 1,)),
            dma((n_cols - 1,)),
            dma((n_cols - 1,)),
            dma((7,)),
        ],
        compiler_params=pltpu.CompilerParams(
            collective_id=0, has_side_effects=True, vmem_limit_bytes=60 * 1024 * 1024
        ),
    )(
        kernel_hat, coefficients, wave_speed_sq, wet_mask, boundary_cell.reshape(1, obs),
        height, flux_x, flux_y, jnp.asarray(forward), jnp.asarray(inverse),
    )


def solution(mesh):
    n_rows, n_cols = mesh.shape["rows"], mesh.shape["cols"]
    return jax.shard_map(
        functools.partial(on_device, n_rows, n_cols),
        mesh=mesh,
        in_specs=(
            P(None, "rows", "cols", None),
            P(None, "cols"),
            P("rows", "cols"),
            P("rows", "cols"),
            P(),
            P("rows", "cols"),
            P("rows", "cols"),
            P("rows", "cols"),
        ),
        out_specs=(P("rows", "cols"), P("rows", "cols"), P("rows", "cols"), P("rows", "cols")),
        check_vma=False,
    )
```

```python
import functools
import math

import jax
import jax.numpy as jnp
import numpy as np
from jax import lax
from jax.experimental import pallas as pl
from jax.experimental.pallas import tpu as pltpu
from jax.sharding import PartitionSpec as P

MESH = pl.DeviceIdType.MESH
GROUP = 8
EDGE = 8
LANE = 128
F32 = jnp.float32
BF16 = jnp.bfloat16


def tables(freq_total, steps, row_devs):
    freq = np.arange(freq_total)
    time = np.arange(steps)
    phase = 2.0 * math.pi * (np.outer(freq, time) % freq_total) / freq_total
    cos = np.cos(phase).reshape(row_devs, -1, GROUP, steps)
    sin = np.sin(phase).reshape(row_devs, -1, GROUP, steps)
    both = np.concatenate([cos, -sin], axis=2).reshape(row_devs, -1, steps)
    forward = both.astype(np.float32)
    inverse = np.swapaxes(both, 1, 2) / freq_total
    high = inverse.astype(np.float32).astype(jnp.bfloat16)
    low = (inverse - high.astype(np.float64)).astype(np.float32).astype(jnp.bfloat16)
    return forward, np.concatenate([high, high, low], axis=2)


def split(value):
    high = value.astype(BF16)
    return high, value - high.astype(F32)


def faces(speed, wet, dim):
    ahead = speed.shape[dim] - 1
    opened = wet * pltpu.roll(wet, ahead, dim)
    return 0.5 * opened, opened * (0.25 * (speed + pltpu.roll(speed, ahead, dim)))


def step_once(surf, qx, qy, speed_sq, wet, face_x, face_y):
    energy = speed_sq * surf
    change = []
    for dim, along, across, (half, damp) in ((1, qx, qy, face_x), (0, qy, qx, face_y)):
        ahead = surf.shape[dim] - 1
        later = lambda v: pltpu.roll(v, ahead, dim)
        mass = half * (along + later(along)) - damp * (later(surf) - surf)
        momentum = half * (energy + later(energy)) - damp * (later(along) - along)
        shear = -damp * (later(across) - across)
        change.append([f - pltpu.roll(f, 1, dim) for f in (mass, momentum, shear)])
    (mass_x, mom_x, shear_x), (mass_y, mom_y, shear_y) = change
    return (
        wet * (surf - 0.25 * (mass_x + mass_y)),
        wet * (qx - 0.25 * (mom_x + shear_y)),
        wet * (qy - 0.25 * (shear_x + mom_y)),
    )


def kernel(
    n_rows, n_cols,
    kern_hbm, coef_hbm, sq_hbm, wet_hbm, cell_hbm, surf_hbm, qx_hbm, qy_hbm, fwd_hbm, inv_hbm,
    series_buf, out_buf,
    kern, coef, fwd, inv, cells, pad, wet_int, wet_pad, corner, corner_wet,
    strip_out, strip_in, spec_out, spec_in, whole_buf, whole_in, late_in,
    mid,
    local_sem, kern_sem, halo_send, halo_recv, spec_send, spec_recv,
    whole_send, whole_recv, late_send, late_recv,
):
    row = lax.axis_index("rows")
    col = lax.axis_index("cols")
    freqs, src, obs = kern.shape[1:]
    groups = freqs // GROUP
    tall, wide = surf_hbm.shape
    points = obs // n_cols
    own_steps = series_buf.shape[0]
    has_n, has_s = row > 0, row < n_rows - 1
    has_w, has_e = col > 0, col < n_cols - 1
    at_edge = row == n_rows - 1

    inputs = [
        pltpu.make_async_copy(coef_hbm, coef, local_sem.at[0]),
        pltpu.make_async_copy(fwd_hbm.at[row], fwd, local_sem.at[1]),
        pltpu.make_async_copy(surf_hbm, pad.at[0, :tall, :wide], local_sem.at[2]),
        pltpu.make_async_copy(qx_hbm, pad.at[1, :tall, :wide], local_sem.at[3]),
        pltpu.make_async_copy(qy_hbm, pad.at[2, :tall, :wide], local_sem.at[4]),
        pltpu.make_async_copy(sq_hbm, pad.at[3, :tall, :wide], local_sem.at[5]),
        pltpu.make_async_copy(wet_hbm, wet_int.at[:tall], local_sem.at[6]),
        pltpu.make_async_copy(inv_hbm.at[row], inv, local_sem.at[7]),
        pltpu.make_async_copy(cell_hbm, cells, local_sem.at[8]),
    ]
    for copy in inputs:
        copy.start()
    chunks = []
    for g in range(groups):
        for part in range(2):
            where = pl.ds(g * GROUP, GROUP)
            copy = pltpu.make_async_copy(
                kern_hbm.at[part, where], kern.at[part, where], kern_sem.at[g, part]
            )
            copy.start()
            chunks.append(copy)

    diagonals = [
        (has_n & has_w, -1, -1), (has_n & has_e, -1, 1),
        (has_s & has_w, 1, -1), (has_s & has_e, 1, 1),
    ]
    barrier = pltpu.get_barrier_semaphore()
    for k in range(1, n_rows):
        pl.semaphore_signal(barrier, 1, device_id=(lax.rem(row + k, n_rows), col), device_id_type=MESH)
    for k in range(1, n_cols):
        pl.semaphore_signal(barrier, 1, device_id=(row, lax.rem(col + k, n_cols)), device_id_type=MESH)
    for exists, dr, dc in diagonals:
        @pl.when(exists)
        def _(dr=dr, dc=dc):
            pl.semaphore_signal(barrier, 1, device_id=(row + dr, col + dc), device_id_type=MESH)

    inputs[0].wait()
    inputs[1].wait()
    spectrum = jnp.dot(
        fwd[...], coef[...], precision=lax.Precision.HIGHEST, preferred_element_type=F32
    )

    for copy in inputs[2:7]:
        copy.wait()
    lane = lax.broadcasted_iota(jnp.int32, (tall, LANE), 1)
    packed = jnp.zeros((tall, LANE), F32)
    for k in range(5):
        if k < 4:
            first, last = pad[k, :tall, :LANE], pad[k, :tall, wide - LANE:wide]
        else:
            first = wet_int[:tall, :LANE].astype(F32)
            last = wet_int[:tall, wide - LANE:wide].astype(F32)
        at = 2 * k
        moved = first if at == 0 else pltpu.roll(first, at, 1)
        packed = jnp.where((lane >= at) & (lane < at + 2), moved, packed)
        at = 16 + 2 * k
        packed = jnp.where(
            (lane >= at) & (lane < at + 2), pltpu.roll(last, at + 2, 1), packed
        )
    strip_out[...] = packed.T[:32]

    pl.semaphore_wait(
        barrier,
        n_rows - 1 + n_cols - 1 + sum(exists.astype(jnp.int32) for exists, _, _ in diagonals),
    )

    def remote(source, target, sems, index, to):
        return pltpu.make_async_remote_copy(
            src_ref=source, dst_ref=target, send_sem=sems[0].at[index], recv_sem=sems[1].at[index],
            device_id=to, device_id_type=MESH,
        )

    halo = (halo_send, halo_recv)
    north = (lax.rem(row + n_rows - 1, n_rows), col)
    south = (lax.rem(row + 1, n_rows), col)
    west = (row, lax.rem(col + n_cols - 1, n_cols))
    east = (row, lax.rem(col + 1, n_cols))
    top, bottom = pl.ds(0, EDGE), pl.ds(tall - EDGE, EDGE)
    south_halo, north_halo = pl.ds(tall, EDGE), pl.ds(tall + EDGE, EDGE)
    body = pl.ds(0, wide)
    moves = [
        (has_n, has_s, [
            remote(pad.at[:, top, body], pad.at[:, south_halo, body], halo, 0, north),
            remote(wet_int.at[top], wet_int.at[south_halo], halo, 1, north)]),
        (has_s, has_n, [
            remote(pad.at[:, bottom, body], pad.at[:, north_halo, body], halo, 2, south),
            remote(wet_int.at[bottom], wet_int.at[north_halo], halo, 3, south)]),
        (has_w, has_e, [remote(strip_out.at[pl.ds(0, 16)], strip_in.at[pl.ds(16, 16)], halo, 4, west)]),
        (has_e, has_w, [remote(strip_out.at[pl.ds(16, 16)], strip_in.at[pl.ds(0, 16)], halo, 5, east)]),
    ]
    for i, (exists, dr, dc) in enumerate(diagonals):
        rows_at = top if dr < 0 else bottom
        cols_at = pl.ds(0, LANE) if dc < 0 else pl.ds(wide - LANE, LANE)
        to = (lax.rem(row + dr + n_rows, n_rows), lax.rem(col + dc + n_cols, n_cols))
        moves.append((exists, diagonals[3 - i][0], [
            remote(pad.at[:, rows_at, cols_at], corner.at[i], halo, 6 + 2 * i, to),
            remote(wet_int.at[rows_at, cols_at], corner_wet.at[i], halo, 7 + 2 * i, to)]))
    for exists, _, copies in moves:
        @pl.when(exists)
        def _(copies=copies):
            for copy in copies:
                copy.start()

    lanes16 = lax.broadcasted_iota(jnp.int32, (2 * GROUP, src), 0) % GROUP
    spec_copies = []
    for g in range(groups):
        mine = spectrum[g * 2 * GROUP:(g + 1) * 2 * GROUP]
        turned = jnp.concatenate([-mine[GROUP:], mine[:GROUP]], axis=0)
        total = None
        for part, value in enumerate((mine, turned)):
            chunks[2 * g + part].wait()
            value = value.astype(BF16).astype(F32)
            if src % LANE == 0:
                left = jnp.concatenate(
                    [jnp.where(lanes16 == j, value, 0.0) for j in range(GROUP)], axis=1
                ).astype(BF16)
                right = kern[part, pl.ds(g * GROUP, GROUP)].reshape(GROUP * src, obs)
                term = jnp.dot(left, right, preferred_element_type=F32)
                total = term if total is None else total + term
            else:
                for j in range(GROUP):
                    term = jnp.dot(
                        jnp.where(lanes16 == j, value, 0.0).astype(BF16),
                        kern[part, g * GROUP + j], preferred_element_type=F32,
                    )
                    total = term if total is None else total + term
        for d in range(n_cols):
            spec_out[d, g] = total[:, d * points:(d + 1) * points]
        for k in range(1, n_cols):
            to = lax.rem(col + k, n_cols)
            copy = remote(
                spec_out.at[to, g], spec_in.at[k - 1, g], (spec_send.at[g], spec_recv.at[g]),
                k - 1, (row, to),
            )
            copy.start()
            spec_copies.append(copy)

    for i, (_, arrives, copies) in enumerate(moves):
        @pl.when(arrives)
        def _(copies=copies):
            for copy in copies:
                copy.wait_recv()

        @pl.when(jnp.logical_not(arrives))
        def _(i=i):
            if i == 0:
                pad[:, south_halo, body] = jnp.zeros((4, EDGE, wide), F32)
                wet_int[south_halo] = jnp.zeros((EDGE, wide), jnp.int32)
            elif i == 1:
                pad[:, north_halo, body] = jnp.zeros((4, EDGE, wide), F32)
                wet_int[north_halo] = jnp.zeros((EDGE, wide), jnp.int32)
            elif i == 2:
                strip_in[pl.ds(16, 16)] = jnp.zeros((16, tall), F32)
            elif i == 3:
                strip_in[pl.ds(0, 16)] = jnp.zeros((16, tall), F32)
            else:
                corner[i - 4] = jnp.zeros((4, EDGE, LANE), F32)
                corner_wet[i - 4] = jnp.zeros((EDGE, LANE), jnp.int32)

    beside = jnp.concatenate([strip_in[...], jnp.zeros((LANE - 32, tall), F32)], axis=0).T
    wet_pad[:, :wide] = wet_int[...].astype(F32)
    near = lax.broadcasted_iota(jnp.int32, (EDGE, LANE), 1) < LANE // 2
    for k in range(5):
        side = jnp.where(
            lane < LANE // 2,
            pltpu.roll(beside, LANE - 16 - 2 * k, 1),
            pltpu.roll(beside, LANE - 2 - 2 * k, 1),
        )
        pick = (lambda i: corner[i, k]) if k < 4 else (lambda i: corner_wet[i].astype(F32))
        low = jnp.where(near, pick(0), pick(1))
        high = jnp.where(near, pick(2), pick(3))
        if k < 4:
            pad[k, :tall, wide:] = side
            pad[k, tall:tall + EDGE, wide:] = low
            pad[k, tall + EDGE:, wide:] = high
        else:
            wet_pad[:tall, wide:] = side
            wet_pad[tall:tall + EDGE, wide:] = low
            wet_pad[tall + EDGE:, wide:] = high

    @pl.when(at_edge)
    def _():
        pad[3, tall:tall + 1, :] = jnp.ones((1, wide + LANE), F32)
        wet_pad[tall:tall + 1, :] = jnp.ones((1, wide + LANE), F32)

    def first_step():
        wet, speed_sq = wet_pad[...], pad[3]
        speed = jnp.sqrt(speed_sq)
        face_x, face_y = faces(speed, wet, 1), faces(speed, wet, 0)
        new = step_once(pad[0], pad[1], pad[2], speed_sq, wet, face_x, face_y)
        for k in range(3):
            mid[k] = new[k]

    def second_step():
        wet, speed_sq = wet_pad[...], pad[3]
        speed = jnp.sqrt(speed_sq)
        face_x, face_y = faces(speed, wet, 1), faces(speed, wet, 0)
        new = step_once(mid[0], mid[1], mid[2], speed_sq, wet, face_x, face_y)
        for k in range(3):
            out_buf[k] = new[k][:tall, :wide]

    first_step()

    for copy in spec_copies:
        copy.wait_recv()
    highs, lows = [], []
    for g in range(groups):
        value = spec_out[col, g]
        for k in range(1, n_cols):
            value = value + spec_in[k - 1, g]
        high, low = split(value)
        highs.append(high)
        lows.append(low.astype(BF16))
    inputs[7].wait()
    whole_buf[...] = jnp.dot(
        inv[...], jnp.concatenate(highs + lows + highs, axis=0), preferred_element_type=F32
    )
    whole_copies = []
    for k in range(1, n_rows):
        to = lax.rem(row + k, n_rows)
        copy = remote(
            whole_buf.at[pl.ds(pl.multiple_of(to * own_steps, own_steps), own_steps)],
            whole_in.at[k - 1], (whole_send, whole_recv), k - 1, (to, col),
        )
        copy.start()
        whole_copies.append(copy)

    second_step()
    inputs[8].wait()

    for copy in whole_copies:
        copy.wait_recv()
    value = whole_buf[pl.ds(pl.multiple_of(row * own_steps, own_steps), own_steps)]
    for k in range(1, n_rows):
        value = value + whole_in[k - 1]
    series_buf[...] = value

    late_copies = [
        remote(
            series_buf.at[pl.ds(own_steps - EDGE, EDGE)], late_in.at[col], (late_send, late_recv),
            k - 1, (row, lax.rem(col + k, n_cols)),
        )
        for k in range(1, n_cols)
    ]

    @pl.when(at_edge)
    def _():
        for copy in late_copies:
            copy.start()
        span = wide + LANE
        place = lax.broadcasted_iota(jnp.int32, (span, obs), 0)
        place = jnp.where(place >= wide + LANE // 2, place - span, place) + col * wide
        chosen = jnp.where(place == cells[...], 1.0, 0.0).astype(BF16)
        late_in[col] = value[own_steps - EDGE:]
        for k in range(1, n_cols):
            come = lax.rem(col + n_cols - k, n_cols)
            remote(
                series_buf.at[pl.ds(own_steps - EDGE, EDGE)], late_in.at[come],
                (late_send, late_recv), k - 1, (row, lax.rem(col + k, n_cols)),
            ).wait_recv()
        latest = jnp.concatenate([late_in[d] for d in range(n_cols)], axis=1)
        high, rest = split(latest)
        middle, rest = split(rest)
        parts = jnp.concatenate([high.astype(F32), middle.astype(F32), rest, rest], axis=0)
        picked = lax.dot_general(
            parts.astype(BF16), chosen, (((1,), (1,)), ((), ())), preferred_element_type=F32
        )
        picked = picked[:EDGE] + picked[EDGE:2 * EDGE] + picked[2 * EDGE:3 * EDGE]
        base = tall - 2 * EDGE
        part_rows = pl.ds(base, 3 * EDGE)
        at_ghost = lax.broadcasted_iota(jnp.int32, (3 * EDGE, span), 0) == 2 * EDGE
        ghosts = [
            jnp.broadcast_to(picked[EDGE - 2 + k:EDGE - 1 + k], (3 * EDGE, span)) for k in range(2)
        ]
        wet, speed_sq = wet_pad[part_rows], pad[3, part_rows]
        speed = jnp.sqrt(speed_sq)
        face_x, face_y = faces(speed, wet, 1), faces(speed, wet, 0)
        surf = jnp.where(at_ghost, ghosts[0], pad[0, part_rows])
        surf, qx, qy = step_once(
            surf, pad[1, part_rows], pad[2, part_rows], speed_sq, wet, face_x, face_y
        )
        surf = jnp.where(at_ghost, ghosts[1], surf)
        qx = jnp.where(at_ghost, 0.0, qx)
        qy = jnp.where(at_ghost, 0.0, qy)
        new = step_once(surf, qx, qy, speed_sq, wet, face_x, face_y)
        for k in range(3):
            out_buf[k, tall - EDGE:] = new[k][EDGE:2 * EDGE, :wide]

    for exists, _, copies in moves:
        @pl.when(exists)
        def _(copies=copies):
            for copy in copies:
                copy.wait_send()
    for copy in spec_copies + whole_copies:
        copy.wait_send()

    @pl.when(at_edge)
    def _():
        for copy in late_copies:
            copy.wait_send()


def write_out(series, fields, series_hbm, surf_hbm, qx_hbm, qy_hbm, sems):
    copies = [pltpu.make_async_copy(series, series_hbm, sems.at[3])]
    for k, target in enumerate((surf_hbm, qx_hbm, qy_hbm)):
        copies.append(pltpu.make_async_copy(fields.at[k], target, sems.at[k]))
    for copy in copies:
        copy.start()
    for copy in copies:
        copy.wait()


def on_device(n_rows, n_cols, kernel_hat, coefficients, wave_speed_sq, wet_mask, boundary_cell, height, flux_x, flux_y):
    _, freqs, src, obs = kernel_hat.shape
    steps = coefficients.shape[0]
    tall, wide = height.shape
    groups = freqs // GROUP
    points = obs // n_cols
    own_steps = steps // n_rows
    span = wide + LANE
    forward, inverse = tables(freqs * n_rows, steps, n_rows)
    dma = pltpu.SemaphoreType.DMA
    anywhere = pl.BlockSpec(memory_space=pltpu.HBM)
    in_vmem = pl.BlockSpec(memory_space=pltpu.VMEM)
    series, fields = pl.pallas_call(
        functools.partial(kernel, n_rows, n_cols),
        out_shape=(
            pltpu.VMEM((own_steps, points), F32),
            pltpu.VMEM((3, tall, wide), F32),
        ),
        in_specs=[anywhere] * 10,
        out_specs=(in_vmem,) * 2,
        scratch_shapes=[
            pltpu.VMEM(kernel_hat.shape, BF16),
            pltpu.VMEM(coefficients.shape, F32),
            pltpu.VMEM(forward.shape[1:], F32),
            pltpu.VMEM(inverse.shape[1:], BF16),
            pltpu.VMEM((1, obs), jnp.int32),
            pltpu.VMEM((4, tall + 2 * EDGE, span), F32),
            pltpu.VMEM((tall + 2 * EDGE, wide), jnp.int32),
            pltpu.VMEM((tall + 2 * EDGE, span), F32),
            pltpu.VMEM((4, 4, EDGE, LANE), F32),
            pltpu.VMEM((4, EDGE, LANE), jnp.int32),
            pltpu.VMEM((32, tall), F32),
            pltpu.VMEM((32, tall), F32),
            pltpu.VMEM((n_cols, groups, 2 * GROUP, points), F32),
            pltpu.VMEM((n_cols - 1, groups, 2 * GROUP, points), F32),
            pltpu.VMEM((steps, points), F32),
            pltpu.VMEM((n_rows - 1, own_steps, points), F32),
            pltpu.VMEM((n_cols, EDGE, points), F32),
            pltpu.VMEM((3, tall + 2 * EDGE, span), F32),
            dma((9,)),
            dma((groups, 2)),
            dma((14,)),
            dma((14,)),
            dma((groups, n_cols - 1)),
            dma((groups, n_cols - 1)),
            dma((n_rows - 1,)),
            dma((n_rows - 1,)),
            dma((n_cols - 1,)),
            dma((n_cols - 1,)),
        ],
        compiler_params=pltpu.CompilerParams(
            collective_id=0, has_side_effects=True, vmem_limit_bytes=60 * 1024 * 1024
        ),
    )(
        kernel_hat, coefficients, wave_speed_sq, wet_mask, boundary_cell.reshape(1, obs),
        height, flux_x, flux_y, jnp.asarray(forward), jnp.asarray(inverse),
    )
    return pl.pallas_call(
        write_out,
        out_shape=(
            jax.ShapeDtypeStruct((own_steps, points), F32),
            jax.ShapeDtypeStruct((tall, wide), F32),
            jax.ShapeDtypeStruct((tall, wide), F32),
            jax.ShapeDtypeStruct((tall, wide), F32),
        ),
        in_specs=[in_vmem] * 2,
        out_specs=(anywhere,) * 4,
        scratch_shapes=[dma((4,))],
        compiler_params=pltpu.CompilerParams(vmem_limit_bytes=4 * 1024 * 1024),
    )(series, fields)


def solution(mesh):
    n_rows, n_cols = mesh.shape["rows"], mesh.shape["cols"]
    return jax.shard_map(
        functools.partial(on_device, n_rows, n_cols),
        mesh=mesh,
        in_specs=(
            P(None, "rows", "cols", None),
            P(None, "cols"),
            P("rows", "cols"),
            P("rows", "cols"),
            P(),
            P("rows", "cols"),
            P("rows", "cols"),
            P("rows", "cols"),
        ),
        out_specs=(P("rows", "cols"), P("rows", "cols"), P("rows", "cols"), P("rows", "cols")),
        check_vma=False,
    )
```

```python
import functools
import math

import jax
import jax.numpy as jnp
import numpy as np
from jax import lax
from jax.experimental import pallas as pl
from jax.experimental.pallas import tpu as pltpu
from jax.sharding import PartitionSpec as P

MESH = pl.DeviceIdType.MESH
GROUP = 8
EDGE = 8
LANE = 128
F32 = jnp.float32
BF16 = jnp.bfloat16


def tables(freq_total, steps, row_devs):
    freq = np.arange(freq_total)
    time = np.arange(steps)
    phase = 2.0 * math.pi * (np.outer(freq, time) % freq_total) / freq_total
    cos = np.cos(phase).reshape(row_devs, -1, GROUP, steps)
    sin = np.sin(phase).reshape(row_devs, -1, GROUP, steps)
    both = np.concatenate([cos, -sin], axis=2).reshape(row_devs, -1, steps)
    forward = both.astype(np.float32)
    inverse = np.swapaxes(both, 1, 2) / freq_total
    high = inverse.astype(np.float32).astype(jnp.bfloat16)
    low = (inverse - high.astype(np.float64)).astype(np.float32).astype(jnp.bfloat16)
    return forward, np.concatenate([high, high, low], axis=2)


def split(value):
    high = value.astype(BF16)
    return high, value - high.astype(F32)


def faces(speed, wet, dim):
    ahead = speed.shape[dim] - 1
    opened = wet * pltpu.roll(wet, ahead, dim)
    return 0.5 * opened, opened * (0.25 * (speed + pltpu.roll(speed, ahead, dim)))


def step_once(surf, qx, qy, speed_sq, wet, face_x, face_y):
    energy = speed_sq * surf
    change = []
    for dim, along, across, (half, damp) in ((1, qx, qy, face_x), (0, qy, qx, face_y)):
        ahead = surf.shape[dim] - 1
        later = lambda v: pltpu.roll(v, ahead, dim)
        mass = half * (along + later(along)) - damp * (later(surf) - surf)
        momentum = half * (energy + later(energy)) - damp * (later(along) - along)
        shear = -damp * (later(across) - across)
        change.append([f - pltpu.roll(f, 1, dim) for f in (mass, momentum, shear)])
    (mass_x, mom_x, shear_x), (mass_y, mom_y, shear_y) = change
    return (
        wet * (surf - 0.25 * (mass_x + mass_y)),
        wet * (qx - 0.25 * (mom_x + shear_y)),
        wet * (qy - 0.25 * (shear_x + mom_y)),
    )


def kernel(
    n_rows, n_cols,
    kern_hbm, coef_hbm, sq_hbm, wet_hbm, cell_hbm, surf_hbm, qx_hbm, qy_hbm, fwd_hbm, inv_hbm,
    series_buf, out_buf,
    kern, coef, fwd, inv, cells, pad, wet_int, wet_pad, corner, corner_wet,
    strip_out, strip_in, spec_out, spec_in, whole_buf, whole_in, late_out, late_in, latest_buf,
    mid, chosen_buf,
    local_sem, kern_sem, halo_send, halo_recv, spec_send, spec_recv,
    whole_send, whole_recv, late_send, late_recv,
):
    row = lax.axis_index("rows")
    col = lax.axis_index("cols")
    freqs, src, obs = kern.shape[1:]
    groups = freqs // GROUP
    tall, wide = surf_hbm.shape
    points = obs // n_cols
    own_steps = series_buf.shape[0]
    has_n, has_s = row > 0, row < n_rows - 1
    has_w, has_e = col > 0, col < n_cols - 1
    at_edge = row == n_rows - 1

    inputs = [
        pltpu.make_async_copy(coef_hbm, coef, local_sem.at[0]),
        pltpu.make_async_copy(fwd_hbm.at[row], fwd, local_sem.at[1]),
        pltpu.make_async_copy(surf_hbm, pad.at[0, :tall, :wide], local_sem.at[2]),
        pltpu.make_async_copy(qx_hbm, pad.at[1, :tall, :wide], local_sem.at[3]),
        pltpu.make_async_copy(qy_hbm, pad.at[2, :tall, :wide], local_sem.at[4]),
        pltpu.make_async_copy(sq_hbm, pad.at[3, :tall, :wide], local_sem.at[5]),
        pltpu.make_async_copy(wet_hbm, wet_int.at[:tall], local_sem.at[6]),
        pltpu.make_async_copy(inv_hbm.at[row], inv, local_sem.at[7]),
        pltpu.make_async_copy(cell_hbm, cells, local_sem.at[8]),
    ]
    for copy in inputs:
        copy.start()
    chunks = []
    for g in range(groups):
        for part in range(2):
            where = pl.ds(g * GROUP, GROUP)
            copy = pltpu.make_async_copy(
                kern_hbm.at[part, where], kern.at[part, where], kern_sem.at[g, part]
            )
            copy.start()
            chunks.append(copy)

    diagonals = [
        (has_n & has_w, -1, -1), (has_n & has_e, -1, 1),
        (has_s & has_w, 1, -1), (has_s & has_e, 1, 1),
    ]
    barrier = pltpu.get_barrier_semaphore()
    for k in range(1, n_rows):
        pl.semaphore_signal(barrier, 1, device_id=(lax.rem(row + k, n_rows), col), device_id_type=MESH)
    for k in range(1, n_cols):
        pl.semaphore_signal(barrier, 1, device_id=(row, lax.rem(col + k, n_cols)), device_id_type=MESH)
    for k in range(1, n_cols):
        other = lax.rem(col + k, n_cols)

        @pl.when(jnp.logical_not(at_edge))
        def _(other=other):
            pl.semaphore_signal(barrier, 1, device_id=(n_rows - 1, other), device_id_type=MESH)

        @pl.when(at_edge)
        def _(other=other):
            for r in range(n_rows - 1):
                pl.semaphore_signal(barrier, 1, device_id=(r, other), device_id_type=MESH)
    for exists, dr, dc in diagonals:
        @pl.when(exists)
        def _(dr=dr, dc=dc):
            pl.semaphore_signal(barrier, 1, device_id=(row + dr, col + dc), device_id_type=MESH)

    inputs[0].wait()
    inputs[1].wait()
    spectrum = jnp.dot(
        fwd[...], coef[...], precision=lax.Precision.HIGHEST, preferred_element_type=F32
    )

    for copy in inputs[2:7]:
        copy.wait()
    lane = lax.broadcasted_iota(jnp.int32, (tall, LANE), 1)
    packed = jnp.zeros((tall, LANE), F32)
    for k in range(5):
        if k < 4:
            first, last = pad[k, :tall, :LANE], pad[k, :tall, wide - LANE:wide]
        else:
            first = wet_int[:tall, :LANE].astype(F32)
            last = wet_int[:tall, wide - LANE:wide].astype(F32)
        at = 2 * k
        moved = first if at == 0 else pltpu.roll(first, at, 1)
        packed = jnp.where((lane >= at) & (lane < at + 2), moved, packed)
        at = 16 + 2 * k
        packed = jnp.where(
            (lane >= at) & (lane < at + 2), pltpu.roll(last, at + 2, 1), packed
        )
    strip_out[...] = packed.T[:32]

    pl.semaphore_wait(
        barrier,
        n_rows - 1 + n_cols - 1
        + (n_cols - 1) * jnp.where(at_edge, n_rows - 1, 1)
        + sum(exists.astype(jnp.int32) for exists, _, _ in diagonals),
    )

    def remote(source, target, sems, index, to):
        return pltpu.make_async_remote_copy(
            src_ref=source, dst_ref=target, send_sem=sems[0].at[index], recv_sem=sems[1].at[index],
            device_id=to, device_id_type=MESH,
        )

    halo = (halo_send, halo_recv)
    north = (lax.rem(row + n_rows - 1, n_rows), col)
    south = (lax.rem(row + 1, n_rows), col)
    west = (row, lax.rem(col + n_cols - 1, n_cols))
    east = (row, lax.rem(col + 1, n_cols))
    top, bottom = pl.ds(0, EDGE), pl.ds(tall - EDGE, EDGE)
    south_halo, north_halo = pl.ds(tall, EDGE), pl.ds(tall + EDGE, EDGE)
    body = pl.ds(0, wide)
    moves = [
        (has_n, has_s, [
            remote(pad.at[:, top, body], pad.at[:, south_halo, body], halo, 0, north),
            remote(wet_int.at[top], wet_int.at[south_halo], halo, 1, north)]),
        (has_s, has_n, [
            remote(pad.at[:, bottom, body], pad.at[:, north_halo, body], halo, 2, south),
            remote(wet_int.at[bottom], wet_int.at[north_halo], halo, 3, south)]),
        (has_w, has_e, [remote(strip_out.at[pl.ds(0, 16)], strip_in.at[pl.ds(16, 16)], halo, 4, west)]),
        (has_e, has_w, [remote(strip_out.at[pl.ds(16, 16)], strip_in.at[pl.ds(0, 16)], halo, 5, east)]),
    ]
    for i, (exists, dr, dc) in enumerate(diagonals):
        rows_at = top if dr < 0 else bottom
        cols_at = pl.ds(0, LANE) if dc < 0 else pl.ds(wide - LANE, LANE)
        to = (lax.rem(row + dr + n_rows, n_rows), lax.rem(col + dc + n_cols, n_cols))
        moves.append((exists, diagonals[3 - i][0], [
            remote(pad.at[:, rows_at, cols_at], corner.at[i], halo, 6 + 2 * i, to),
            remote(wet_int.at[rows_at, cols_at], corner_wet.at[i], halo, 7 + 2 * i, to)]))
    for exists, _, copies in moves:
        @pl.when(exists)
        def _(copies=copies):
            for copy in copies:
                copy.start()

    lanes16 = lax.broadcasted_iota(jnp.int32, (2 * GROUP, src), 0) % GROUP
    spec_copies = []
    for g in range(groups):
        mine = spectrum[g * 2 * GROUP:(g + 1) * 2 * GROUP]
        turned = jnp.concatenate([-mine[GROUP:], mine[:GROUP]], axis=0)
        total = None
        chunks[2 * g].wait()
        chunks[2 * g + 1].wait()
        for part, value in enumerate((mine, turned)):
            value = value.astype(BF16).astype(F32)
            if src % LANE == 0:
                left = jnp.concatenate(
                    [jnp.where(lanes16 == j, value, 0.0) for j in range(GROUP)], axis=1
                ).astype(BF16)
                right = kern[part, pl.ds(g * GROUP, GROUP)].reshape(GROUP * src, obs)
                term = jnp.dot(left, right, preferred_element_type=F32)
                total = term if total is None else total + term
            else:
                for j in range(GROUP):
                    term = jnp.dot(
                        jnp.where(lanes16 == j, value, 0.0).astype(BF16),
                        kern[part, g * GROUP + j], preferred_element_type=F32,
                    )
                    total = term if total is None else total + term
        for d in range(n_cols):
            spec_out[d, g] = total[:, d * points:(d + 1) * points]
        for k in range(1, n_cols):
            to = lax.rem(col + k, n_cols)
            copy = remote(
                spec_out.at[to, g], spec_in.at[k - 1, g], (spec_send.at[g], spec_recv.at[g]),
                k - 1, (row, to),
            )
            copy.start()
            spec_copies.append(copy)

    for i, (_, arrives, copies) in enumerate(moves):
        @pl.when(arrives)
        def _(copies=copies):
            for copy in copies:
                copy.wait_recv()

        @pl.when(jnp.logical_not(arrives))
        def _(i=i):
            if i == 0:
                pad[:, south_halo, body] = jnp.zeros((4, EDGE, wide), F32)
                wet_int[south_halo] = jnp.zeros((EDGE, wide), jnp.int32)
            elif i == 1:
                pad[:, north_halo, body] = jnp.zeros((4, EDGE, wide), F32)
                wet_int[north_halo] = jnp.zeros((EDGE, wide), jnp.int32)
            elif i == 2:
                strip_in[pl.ds(16, 16)] = jnp.zeros((16, tall), F32)
            elif i == 3:
                strip_in[pl.ds(0, 16)] = jnp.zeros((16, tall), F32)
            else:
                corner[i - 4] = jnp.zeros((4, EDGE, LANE), F32)
                corner_wet[i - 4] = jnp.zeros((EDGE, LANE), jnp.int32)

    beside = jnp.concatenate([strip_in[...], jnp.zeros((LANE - 32, tall), F32)], axis=0).T
    wet_pad[:, :wide] = wet_int[...].astype(F32)
    near = lax.broadcasted_iota(jnp.int32, (EDGE, LANE), 1) < LANE // 2
    for k in range(5):
        side = jnp.where(
            lane < LANE // 2,
            pltpu.roll(beside, LANE - 16 - 2 * k, 1),
            pltpu.roll(beside, LANE - 2 - 2 * k, 1),
        )
        pick = (lambda i: corner[i, k]) if k < 4 else (lambda i: corner_wet[i].astype(F32))
        low = jnp.where(near, pick(0), pick(1))
        high = jnp.where(near, pick(2), pick(3))
        if k < 4:
            pad[k, :tall, wide:] = side
            pad[k, tall:tall + EDGE, wide:] = low
            pad[k, tall + EDGE:, wide:] = high
        else:
            wet_pad[:tall, wide:] = side
            wet_pad[tall:tall + EDGE, wide:] = low
            wet_pad[tall + EDGE:, wide:] = high

    @pl.when(at_edge)
    def _():
        pad[3, tall:tall + 1, :] = jnp.ones((1, wide + LANE), F32)
        wet_pad[tall:tall + 1, :] = jnp.ones((1, wide + LANE), F32)

    def first_step():
        wet, speed_sq = wet_pad[...], pad[3]
        speed = jnp.sqrt(speed_sq)
        face_x, face_y = faces(speed, wet, 1), faces(speed, wet, 0)
        new = step_once(pad[0], pad[1], pad[2], speed_sq, wet, face_x, face_y)
        for k in range(3):
            mid[k] = new[k]

    def second_step():
        wet, speed_sq = wet_pad[...], pad[3]
        speed = jnp.sqrt(speed_sq)
        face_x, face_y = faces(speed, wet, 1), faces(speed, wet, 0)
        new = step_once(mid[0], mid[1], mid[2], speed_sq, wet, face_x, face_y)
        for k in range(3):
            out_buf[k] = new[k][:tall, :wide]

    first_step()

    for copy in spec_copies:
        copy.wait_recv()
    highs, lows = [], []
    for g in range(groups):
        value = spec_out[col, g]
        for k in range(1, n_cols):
            value = value + spec_in[k - 1, g]
        high, low = split(value)
        highs.append(high)
        lows.append(low.astype(BF16))
    inputs[7].wait()
    whole = jnp.dot(
        inv[...], jnp.concatenate(highs + lows + highs, axis=0), preferred_element_type=F32
    )
    late_out[...] = whole[whole.shape[0] - 2:]
    whole_buf[...] = whole
    late_copies = []
    for k in range(1, n_cols):
        copy = pltpu.make_async_remote_copy(
            src_ref=late_out, dst_ref=late_in.at[k - 1, row],
            send_sem=late_send.at[k - 1], recv_sem=late_recv.at[k - 1, row],
            device_id=(n_rows - 1, lax.rem(col + k, n_cols)), device_id_type=MESH,
        )
        copy.start()
        late_copies.append(copy)
    whole_copies = []
    for k in range(1, n_rows):
        to = lax.rem(row + k, n_rows)
        copy = remote(
            whole_buf.at[pl.ds(pl.multiple_of(to * own_steps, own_steps), own_steps)],
            whole_in.at[k - 1], (whole_send, whole_recv), k - 1, (to, col),
        )
        copy.start()
        whole_copies.append(copy)

    second_step()
    inputs[8].wait()
    span = wide + LANE

    @pl.when(at_edge)
    def _():
        place = lax.broadcasted_iota(jnp.int32, (span, obs), 0)
        place = jnp.where(place >= wide + LANE // 2, place - span, place) + col * wide
        chosen_buf[...] = jnp.where(place == cells[...], 1.0, 0.0).astype(BF16)

    for copy in whole_copies:
        copy.wait_recv()
    value = whole_buf[pl.ds(pl.multiple_of(row * own_steps, own_steps), own_steps)]
    for k in range(1, n_rows):
        value = value + whole_in[k - 1]
    series_buf[...] = value

    @pl.when(at_edge)
    def _():
        latest_buf[col] = value[own_steps - 2:]
        for k in range(1, n_cols):
            share = None
            for r in range(n_rows):
                pltpu.make_async_remote_copy(
                    src_ref=late_out, dst_ref=late_in.at[k - 1, r],
                    send_sem=late_send.at[k - 1], recv_sem=late_recv.at[k - 1, r],
                    device_id=(row, lax.rem(col + k, n_cols)), device_id_type=MESH,
                ).wait_recv()
                share = late_in[k - 1, r] if share is None else share + late_in[k - 1, r]
            latest_buf[lax.rem(col + n_cols - k, n_cols)] = share
        latest = jnp.concatenate([latest_buf[d] for d in range(n_cols)], axis=1)
        high, rest = split(latest)
        middle, rest = split(rest)
        parts = jnp.concatenate([high.astype(F32), middle.astype(F32), rest, rest], axis=0)
        picked = lax.dot_general(
            parts.astype(BF16), chosen_buf[...], (((1,), (1,)), ((), ())),
            preferred_element_type=F32,
        )
        picked = picked[0:2] + picked[2:4] + picked[4:6]
        base = tall - 2 * EDGE
        part_rows = pl.ds(base, 3 * EDGE)
        at_ghost = lax.broadcasted_iota(jnp.int32, (3 * EDGE, span), 0) == 2 * EDGE
        ghosts = [
            jnp.broadcast_to(picked[k:k + 1], (3 * EDGE, span)) for k in range(2)
        ]
        wet, speed_sq = wet_pad[part_rows], pad[3, part_rows]
        speed = jnp.sqrt(speed_sq)
        face_x, face_y = faces(speed, wet, 1), faces(speed, wet, 0)
        surf = jnp.where(at_ghost, ghosts[0], pad[0, part_rows])
        surf, qx, qy = step_once(
            surf, pad[1, part_rows], pad[2, part_rows], speed_sq, wet, face_x, face_y
        )
        surf = jnp.where(at_ghost, ghosts[1], surf)
        qx = jnp.where(at_ghost, 0.0, qx)
        qy = jnp.where(at_ghost, 0.0, qy)
        new = step_once(surf, qx, qy, speed_sq, wet, face_x, face_y)
        for k in range(3):
            out_buf[k, tall - EDGE:] = new[k][EDGE:2 * EDGE, :wide]

    for exists, _, copies in moves:
        @pl.when(exists)
        def _(copies=copies):
            for copy in copies:
                copy.wait_send()
    for copy in spec_copies + whole_copies + late_copies:
        copy.wait_send()


def write_out(series, fields, series_hbm, surf_hbm, qx_hbm, qy_hbm, sems):
    copies = [pltpu.make_async_copy(series, series_hbm, sems.at[3])]
    for k, target in enumerate((surf_hbm, qx_hbm, qy_hbm)):
        copies.append(pltpu.make_async_copy(fields.at[k], target, sems.at[k]))
    for copy in copies:
        copy.start()
    for copy in copies:
        copy.wait()


def on_device(n_rows, n_cols, kernel_hat, coefficients, wave_speed_sq, wet_mask, boundary_cell, height, flux_x, flux_y):
    _, freqs, src, obs = kernel_hat.shape
    steps = coefficients.shape[0]
    tall, wide = height.shape
    groups = freqs // GROUP
    points = obs // n_cols
    own_steps = steps // n_rows
    span = wide + LANE
    forward, inverse = tables(freqs * n_rows, steps, n_rows)
    dma = pltpu.SemaphoreType.DMA
    anywhere = pl.BlockSpec(memory_space=pltpu.HBM)
    in_vmem = pl.BlockSpec(memory_space=pltpu.VMEM)
    series, fields = pl.pallas_call(
        functools.partial(kernel, n_rows, n_cols),
        out_shape=(
            pltpu.VMEM((own_steps, points), F32),
            pltpu.VMEM((3, tall, wide), F32),
        ),
        in_specs=[anywhere] * 10,
        out_specs=(in_vmem,) * 2,
        scratch_shapes=[
            pltpu.VMEM(kernel_hat.shape, BF16),
            pltpu.VMEM(coefficients.shape, F32),
            pltpu.VMEM(forward.shape[1:], F32),
            pltpu.VMEM(inverse.shape[1:], BF16),
            pltpu.VMEM((1, obs), jnp.int32),
            pltpu.VMEM((4, tall + 2 * EDGE, span), F32),
            pltpu.VMEM((tall + 2 * EDGE, wide), jnp.int32),
            pltpu.VMEM((tall + 2 * EDGE, span), F32),
            pltpu.VMEM((4, 4, EDGE, LANE), F32),
            pltpu.VMEM((4, EDGE, LANE), jnp.int32),
            pltpu.VMEM((32, tall), F32),
            pltpu.VMEM((32, tall), F32),
            pltpu.VMEM((n_cols, groups, 2 * GROUP, points), F32),
            pltpu.VMEM((n_cols - 1, groups, 2 * GROUP, points), F32),
            pltpu.VMEM((steps, points), F32),
            pltpu.VMEM((n_rows - 1, own_steps, points), F32),
            pltpu.VMEM((2, points), F32),
            pltpu.VMEM((n_cols - 1, n_rows, 2, points), F32),
            pltpu.VMEM((n_cols, 2, points), F32),
            pltpu.VMEM((3, tall + 2 * EDGE, span), F32),
            pltpu.VMEM((span, obs), BF16),
            dma((9,)),
            dma((groups, 2)),
            dma((14,)),
            dma((14,)),
            dma((groups, n_cols - 1)),
            dma((groups, n_cols - 1)),
            dma((n_rows - 1,)),
            dma((n_rows - 1,)),
            dma((n_cols - 1,)),
            dma((n_cols - 1, n_rows)),
        ],
        compiler_params=pltpu.CompilerParams(
            collective_id=0, has_side_effects=True, vmem_limit_bytes=60 * 1024 * 1024
        ),
    )(
        kernel_hat, coefficients, wave_speed_sq, wet_mask, boundary_cell.reshape(1, obs),
        height, flux_x, flux_y, jnp.asarray(forward), jnp.asarray(inverse),
    )
    return pl.pallas_call(
        write_out,
        out_shape=(
            jax.ShapeDtypeStruct((own_steps, points), F32),
            jax.ShapeDtypeStruct((tall, wide), F32),
            jax.ShapeDtypeStruct((tall, wide), F32),
            jax.ShapeDtypeStruct((tall, wide), F32),
        ),
        in_specs=[in_vmem] * 2,
        out_specs=(anywhere,) * 4,
        scratch_shapes=[dma((4,))],
        compiler_params=pltpu.CompilerParams(vmem_limit_bytes=4 * 1024 * 1024),
    )(series, fields)


def solution(mesh):
    n_rows, n_cols = mesh.shape["rows"], mesh.shape["cols"]
    return jax.shard_map(
        functools.partial(on_device, n_rows, n_cols),
        mesh=mesh,
        in_specs=(
            P(None, "rows", "cols", None),
            P(None, "cols"),
            P("rows", "cols"),
            P("rows", "cols"),
            P(),
            P("rows", "cols"),
            P("rows", "cols"),
            P("rows", "cols"),
        ),
        out_specs=(P("rows", "cols"), P("rows", "cols"), P("rows", "cols"), P("rows", "cols")),
        check_vma=False,
    )
```

```python
import functools
import math

import jax
import jax.numpy as jnp
import numpy as np
from jax import lax
from jax.experimental import pallas as pl
from jax.experimental.pallas import tpu as pltpu
from jax.sharding import PartitionSpec as P

MESH = pl.DeviceIdType.MESH
GROUP = 8
EDGE = 8
LANE = 128
F32 = jnp.float32
BF16 = jnp.bfloat16


def tables(freq_total, steps, row_devs):
    freq = np.arange(freq_total)
    time = np.arange(steps)
    phase = 2.0 * math.pi * (np.outer(freq, time) % freq_total) / freq_total
    cos = np.cos(phase).reshape(row_devs, -1, GROUP, steps)
    sin = np.sin(phase).reshape(row_devs, -1, GROUP, steps)
    both = np.concatenate([cos, -sin], axis=2).reshape(row_devs, -1, steps)
    forward = both.astype(np.float32)
    inverse = np.swapaxes(both, 1, 2) / freq_total
    high = inverse.astype(np.float32).astype(jnp.bfloat16)
    low = (inverse - high.astype(np.float64)).astype(np.float32).astype(jnp.bfloat16)
    return forward, np.concatenate([high, high, low], axis=2)


def split(value):
    high = value.astype(BF16)
    return high, value - high.astype(F32)


def faces(speed, wet, dim):
    ahead = speed.shape[dim] - 1
    opened = wet * pltpu.roll(wet, ahead, dim)
    return 0.5 * opened, opened * (0.25 * (speed + pltpu.roll(speed, ahead, dim)))


def step_once(surf, qx, qy, speed_sq, wet, face_x, face_y):
    energy = speed_sq * surf
    change = []
    for dim, along, across, (half, damp) in ((1, qx, qy, face_x), (0, qy, qx, face_y)):
        ahead = surf.shape[dim] - 1
        later = lambda v: pltpu.roll(v, ahead, dim)
        mass = half * (along + later(along)) - damp * (later(surf) - surf)
        momentum = half * (energy + later(energy)) - damp * (later(along) - along)
        shear = -damp * (later(across) - across)
        change.append([f - pltpu.roll(f, 1, dim) for f in (mass, momentum, shear)])
    (mass_x, mom_x, shear_x), (mass_y, mom_y, shear_y) = change
    return (
        wet * (surf - 0.25 * (mass_x + mass_y)),
        wet * (qx - 0.25 * (mom_x + shear_y)),
        wet * (qy - 0.25 * (shear_x + mom_y)),
    )


def kernel(
    n_rows, n_cols,
    kern_hbm, coef_hbm, sq_hbm, wet_hbm, cell_hbm, surf_hbm, qx_hbm, qy_hbm, fwd_hbm, inv_hbm,
    series_buf, out_buf,
    kern, coef, fwd, inv, cells, pad, wet_int, wet_pad, corner, corner_wet,
    strip_out, strip_in, spec_out, spec_in, whole_buf, whole_in, late_out, late_in, latest_buf,
    mid, chosen_buf,
    local_sem, kern_sem, halo_send, halo_recv, spec_send, spec_recv,
    whole_send, whole_recv, late_send, late_recv,
):
    row = lax.axis_index("rows")
    col = lax.axis_index("cols")
    freqs, src, obs = kern.shape[1:]
    groups = freqs // GROUP
    tall, wide = surf_hbm.shape
    points = obs // n_cols
    own_steps = series_buf.shape[0]
    has_n, has_s = row > 0, row < n_rows - 1
    has_w, has_e = col > 0, col < n_cols - 1
    at_edge = row == n_rows - 1

    inputs = [
        pltpu.make_async_copy(coef_hbm, coef, local_sem.at[0]),
        pltpu.make_async_copy(fwd_hbm.at[row], fwd, local_sem.at[1]),
        pltpu.make_async_copy(surf_hbm, pad.at[0, :tall, :wide], local_sem.at[2]),
        pltpu.make_async_copy(qx_hbm, pad.at[1, :tall, :wide], local_sem.at[3]),
        pltpu.make_async_copy(qy_hbm, pad.at[2, :tall, :wide], local_sem.at[4]),
        pltpu.make_async_copy(sq_hbm, pad.at[3, :tall, :wide], local_sem.at[5]),
        pltpu.make_async_copy(wet_hbm, wet_int.at[:tall], local_sem.at[6]),
        pltpu.make_async_copy(inv_hbm.at[row], inv, local_sem.at[7]),
        pltpu.make_async_copy(cell_hbm, cells, local_sem.at[8]),
    ]
    for copy in inputs:
        copy.start()
    chunks = []
    for g in range(groups):
        for part in range(2):
            where = pl.ds(g * GROUP, GROUP)
            copy = pltpu.make_async_copy(
                kern_hbm.at[part, where], kern.at[part, where], kern_sem.at[g, part]
            )
            copy.start()
            chunks.append(copy)

    diagonals = [
        (has_n & has_w, -1, -1), (has_n & has_e, -1, 1),
        (has_s & has_w, 1, -1), (has_s & has_e, 1, 1),
    ]
    barrier = pltpu.get_barrier_semaphore()
    for k in range(1, n_rows):
        pl.semaphore_signal(barrier, 1, device_id=(lax.rem(row + k, n_rows), col), device_id_type=MESH)
    for k in range(1, n_cols):
        pl.semaphore_signal(barrier, 1, device_id=(row, lax.rem(col + k, n_cols)), device_id_type=MESH)
    for k in range(1, n_cols):
        other = lax.rem(col + k, n_cols)

        @pl.when(jnp.logical_not(at_edge))
        def _(other=other):
            pl.semaphore_signal(barrier, 1, device_id=(n_rows - 1, other), device_id_type=MESH)

        @pl.when(at_edge)
        def _(other=other):
            for r in range(n_rows - 1):
                pl.semaphore_signal(barrier, 1, device_id=(r, other), device_id_type=MESH)
    for exists, dr, dc in diagonals:
        @pl.when(exists)
        def _(dr=dr, dc=dc):
            pl.semaphore_signal(barrier, 1, device_id=(row + dr, col + dc), device_id_type=MESH)

    inputs[0].wait()
    inputs[1].wait()
    spectrum = jnp.dot(
        fwd[...], coef[...], precision=lax.Precision.HIGHEST, preferred_element_type=F32
    )

    for copy in inputs[2:7]:
        copy.wait()
    lane = lax.broadcasted_iota(jnp.int32, (tall, LANE), 1)
    packed = jnp.zeros((tall, LANE), F32)
    for k in range(5):
        if k < 4:
            first, last = pad[k, :tall, :LANE], pad[k, :tall, wide - LANE:wide]
        else:
            first = wet_int[:tall, :LANE].astype(F32)
            last = wet_int[:tall, wide - LANE:wide].astype(F32)
        at = 2 * k
        moved = first if at == 0 else pltpu.roll(first, at, 1)
        packed = jnp.where((lane >= at) & (lane < at + 2), moved, packed)
        at = 16 + 2 * k
        packed = jnp.where(
            (lane >= at) & (lane < at + 2), pltpu.roll(last, at + 2, 1), packed
        )
    strip_out[...] = packed.T[:32]

    def remote(source, target, sems, index, to):
        return pltpu.make_async_remote_copy(
            src_ref=source, dst_ref=target, send_sem=sems[0].at[index], recv_sem=sems[1].at[index],
            device_id=to, device_id_type=MESH,
        )

    halo = (halo_send, halo_recv)
    north = (lax.rem(row + n_rows - 1, n_rows), col)
    south = (lax.rem(row + 1, n_rows), col)
    west = (row, lax.rem(col + n_cols - 1, n_cols))
    east = (row, lax.rem(col + 1, n_cols))
    top, bottom = pl.ds(0, EDGE), pl.ds(tall - EDGE, EDGE)
    south_halo, north_halo = pl.ds(tall, EDGE), pl.ds(tall + EDGE, EDGE)
    body = pl.ds(0, wide)
    moves = [
        (has_n, has_s, [
            remote(pad.at[:, top, body], pad.at[:, south_halo, body], halo, 0, north),
            remote(wet_int.at[top], wet_int.at[south_halo], halo, 1, north)]),
        (has_s, has_n, [
            remote(pad.at[:, bottom, body], pad.at[:, north_halo, body], halo, 2, south),
            remote(wet_int.at[bottom], wet_int.at[north_halo], halo, 3, south)]),
        (has_w, has_e, [remote(strip_out.at[pl.ds(0, 16)], strip_in.at[pl.ds(16, 16)], halo, 4, west)]),
        (has_e, has_w, [remote(strip_out.at[pl.ds(16, 16)], strip_in.at[pl.ds(0, 16)], halo, 5, east)]),
    ]
    for i, (exists, dr, dc) in enumerate(diagonals):
        rows_at = top if dr < 0 else bottom
        cols_at = pl.ds(0, LANE) if dc < 0 else pl.ds(wide - LANE, LANE)
        to = (lax.rem(row + dr + n_rows, n_rows), lax.rem(col + dc + n_cols, n_cols))
        moves.append((exists, diagonals[3 - i][0], [
            remote(pad.at[:, rows_at, cols_at], corner.at[i], halo, 6 + 2 * i, to),
            remote(wet_int.at[rows_at, cols_at], corner_wet.at[i], halo, 7 + 2 * i, to)]))
    lanes16 = lax.broadcasted_iota(jnp.int32, (2 * GROUP, src), 0) % GROUP
    spec_copies, ready = [], []
    for g in range(groups):
        mine = spectrum[g * 2 * GROUP:(g + 1) * 2 * GROUP]
        turned = jnp.concatenate([-mine[GROUP:], mine[:GROUP]], axis=0)
        total = None
        chunks[2 * g].wait()
        chunks[2 * g + 1].wait()
        for part, value in enumerate((mine, turned)):
            value = value.astype(BF16).astype(F32)
            if src % LANE == 0:
                left = jnp.concatenate(
                    [jnp.where(lanes16 == j, value, 0.0) for j in range(GROUP)], axis=1
                ).astype(BF16)
                right = kern[part, pl.ds(g * GROUP, GROUP)].reshape(GROUP * src, obs)
                term = jnp.dot(left, right, preferred_element_type=F32)
                total = term if total is None else total + term
            else:
                for j in range(GROUP):
                    term = jnp.dot(
                        jnp.where(lanes16 == j, value, 0.0).astype(BF16),
                        kern[part, g * GROUP + j], preferred_element_type=F32,
                    )
                    total = term if total is None else total + term
        for d in range(n_cols):
            spec_out[d, g] = total[:, d * points:(d + 1) * points]
        ready.append(g)
        if g < groups // 2 - 1:
            continue
        if g == max(groups // 2 - 1, 0):
            pl.semaphore_wait(
                barrier,
                n_rows - 1 + n_cols - 1
                + (n_cols - 1) * jnp.where(at_edge, n_rows - 1, 1)
                + sum(exists.astype(jnp.int32) for exists, _, _ in diagonals),
            )
            for exists, _, copies in moves:
                @pl.when(exists)
                def _(copies=copies):
                    for copy in copies:
                        copy.start()
        for sent in ready:
            for k in range(1, n_cols):
                to = lax.rem(col + k, n_cols)
                copy = remote(
                    spec_out.at[to, sent], spec_in.at[k - 1, sent],
                    (spec_send.at[sent], spec_recv.at[sent]), k - 1, (row, to),
                )
                copy.start()
                spec_copies.append(copy)
        ready = []

    for i, (_, arrives, copies) in enumerate(moves):
        @pl.when(arrives)
        def _(copies=copies):
            for copy in copies:
                copy.wait_recv()

        @pl.when(jnp.logical_not(arrives))
        def _(i=i):
            if i == 0:
                pad[:, south_halo, body] = jnp.zeros((4, EDGE, wide), F32)
                wet_int[south_halo] = jnp.zeros((EDGE, wide), jnp.int32)
            elif i == 1:
                pad[:, north_halo, body] = jnp.zeros((4, EDGE, wide), F32)
                wet_int[north_halo] = jnp.zeros((EDGE, wide), jnp.int32)
            elif i == 2:
                strip_in[pl.ds(16, 16)] = jnp.zeros((16, tall), F32)
            elif i == 3:
                strip_in[pl.ds(0, 16)] = jnp.zeros((16, tall), F32)
            else:
                corner[i - 4] = jnp.zeros((4, EDGE, LANE), F32)
                corner_wet[i - 4] = jnp.zeros((EDGE, LANE), jnp.int32)

    beside = jnp.concatenate([strip_in[...], jnp.zeros((LANE - 32, tall), F32)], axis=0).T
    wet_pad[:, :wide] = wet_int[...].astype(F32)
    near = lax.broadcasted_iota(jnp.int32, (EDGE, LANE), 1) < LANE // 2
    for k in range(5):
        side = jnp.where(
            lane < LANE // 2,
            pltpu.roll(beside, LANE - 16 - 2 * k, 1),
            pltpu.roll(beside, LANE - 2 - 2 * k, 1),
        )
        pick = (lambda i: corner[i, k]) if k < 4 else (lambda i: corner_wet[i].astype(F32))
        low = jnp.where(near, pick(0), pick(1))
        high = jnp.where(near, pick(2), pick(3))
        if k < 4:
            pad[k, :tall, wide:] = side
            pad[k, tall:tall + EDGE, wide:] = low
            pad[k, tall + EDGE:, wide:] = high
        else:
            wet_pad[:tall, wide:] = side
            wet_pad[tall:tall + EDGE, wide:] = low
            wet_pad[tall + EDGE:, wide:] = high

    @pl.when(at_edge)
    def _():
        pad[3, tall:tall + 1, :] = jnp.ones((1, wide + LANE), F32)
        wet_pad[tall:tall + 1, :] = jnp.ones((1, wide + LANE), F32)

    def first_step():
        wet, speed_sq = wet_pad[...], pad[3]
        speed = jnp.sqrt(speed_sq)
        face_x, face_y = faces(speed, wet, 1), faces(speed, wet, 0)
        new = step_once(pad[0], pad[1], pad[2], speed_sq, wet, face_x, face_y)
        for k in range(3):
            mid[k] = new[k]

    def second_step():
        wet, speed_sq = wet_pad[...], pad[3]
        speed = jnp.sqrt(speed_sq)
        face_x, face_y = faces(speed, wet, 1), faces(speed, wet, 0)
        new = step_once(mid[0], mid[1], mid[2], speed_sq, wet, face_x, face_y)
        for k in range(3):
            out_buf[k] = new[k][:tall, :wide]

    first_step()

    for copy in spec_copies:
        copy.wait_recv()
    highs, lows = [], []
    for g in range(groups):
        value = spec_out[col, g]
        for k in range(1, n_cols):
            value = value + spec_in[k - 1, g]
        high, low = split(value)
        highs.append(high)
        lows.append(low.astype(BF16))
    inputs[7].wait()
    whole = jnp.dot(
        inv[...], jnp.concatenate(highs + lows + highs, axis=0), preferred_element_type=F32
    )
    late_out[...] = whole[whole.shape[0] - 2:]
    whole_buf[...] = whole
    late_copies = []
    for k in range(1, n_cols):
        copy = pltpu.make_async_remote_copy(
            src_ref=late_out, dst_ref=late_in.at[k - 1, row],
            send_sem=late_send.at[k - 1], recv_sem=late_recv.at[k - 1, row],
            device_id=(n_rows - 1, lax.rem(col + k, n_cols)), device_id_type=MESH,
        )
        copy.start()
        late_copies.append(copy)
    whole_copies = []
    for k in range(1, n_rows):
        to = lax.rem(row + k, n_rows)
        copy = remote(
            whole_buf.at[pl.ds(pl.multiple_of(to * own_steps, own_steps), own_steps)],
            whole_in.at[k - 1], (whole_send, whole_recv), k - 1, (to, col),
        )
        copy.start()
        whole_copies.append(copy)

    second_step()
    inputs[8].wait()
    span = wide + LANE

    @pl.when(at_edge)
    def _():
        place = lax.broadcasted_iota(jnp.int32, (span, obs), 0)
        place = jnp.where(place >= wide + LANE // 2, place - span, place) + col * wide
        chosen_buf[...] = jnp.where(place == cells[...], 1.0, 0.0).astype(BF16)

    for copy in whole_copies:
        copy.wait_recv()
    value = whole_buf[pl.ds(pl.multiple_of(row * own_steps, own_steps), own_steps)]
    for k in range(1, n_rows):
        value = value + whole_in[k - 1]
    series_buf[...] = value

    @pl.when(at_edge)
    def _():
        latest_buf[col] = value[own_steps - 2:]
        for k in range(1, n_cols):
            share = None
            for r in range(n_rows):
                pltpu.make_async_remote_copy(
                    src_ref=late_out, dst_ref=late_in.at[k - 1, r],
                    send_sem=late_send.at[k - 1], recv_sem=late_recv.at[k - 1, r],
                    device_id=(row, lax.rem(col + k, n_cols)), device_id_type=MESH,
                ).wait_recv()
                share = late_in[k - 1, r] if share is None else share + late_in[k - 1, r]
            latest_buf[lax.rem(col + n_cols - k, n_cols)] = share
        latest = jnp.concatenate([latest_buf[d] for d in range(n_cols)], axis=1)
        high, rest = split(latest)
        middle, rest = split(rest)
        parts = jnp.concatenate([high.astype(F32), middle.astype(F32), rest, rest], axis=0)
        picked = lax.dot_general(
            parts.astype(BF16), chosen_buf[...], (((1,), (1,)), ((), ())),
            preferred_element_type=F32,
        )
        picked = picked[0:2] + picked[2:4] + picked[4:6]
        base = tall - 2 * EDGE
        part_rows = pl.ds(base, 3 * EDGE)
        at_ghost = lax.broadcasted_iota(jnp.int32, (3 * EDGE, span), 0) == 2 * EDGE
        ghosts = [
            jnp.broadcast_to(picked[k:k + 1], (3 * EDGE, span)) for k in range(2)
        ]
        wet, speed_sq = wet_pad[part_rows], pad[3, part_rows]
        speed = jnp.sqrt(speed_sq)
        face_x, face_y = faces(speed, wet, 1), faces(speed, wet, 0)
        surf = jnp.where(at_ghost, ghosts[0], pad[0, part_rows])
        surf, qx, qy = step_once(
            surf, pad[1, part_rows], pad[2, part_rows], speed_sq, wet, face_x, face_y
        )
        surf = jnp.where(at_ghost, ghosts[1], surf)
        qx = jnp.where(at_ghost, 0.0, qx)
        qy = jnp.where(at_ghost, 0.0, qy)
        new = step_once(surf, qx, qy, speed_sq, wet, face_x, face_y)
        for k in range(3):
            out_buf[k, tall - EDGE:] = new[k][EDGE:2 * EDGE, :wide]

    for exists, _, copies in moves:
        @pl.when(exists)
        def _(copies=copies):
            for copy in copies:
                copy.wait_send()
    for copy in spec_copies + whole_copies + late_copies:
        copy.wait_send()


def write_out(series, fields, series_hbm, surf_hbm, qx_hbm, qy_hbm, sems):
    copies = [pltpu.make_async_copy(series, series_hbm, sems.at[3])]
    for k, target in enumerate((surf_hbm, qx_hbm, qy_hbm)):
        copies.append(pltpu.make_async_copy(fields.at[k], target, sems.at[k]))
    for copy in copies:
        copy.start()
    for copy in copies:
        copy.wait()


def on_device(n_rows, n_cols, kernel_hat, coefficients, wave_speed_sq, wet_mask, boundary_cell, height, flux_x, flux_y):
    _, freqs, src, obs = kernel_hat.shape
    steps = coefficients.shape[0]
    tall, wide = height.shape
    groups = freqs // GROUP
    points = obs // n_cols
    own_steps = steps // n_rows
    span = wide + LANE
    forward, inverse = tables(freqs * n_rows, steps, n_rows)
    dma = pltpu.SemaphoreType.DMA
    anywhere = pl.BlockSpec(memory_space=pltpu.HBM)
    in_vmem = pl.BlockSpec(memory_space=pltpu.VMEM)
    series, fields = pl.pallas_call(
        functools.partial(kernel, n_rows, n_cols),
        out_shape=(
            pltpu.VMEM((own_steps, points), F32),
            pltpu.VMEM((3, tall, wide), F32),
        ),
        in_specs=[anywhere] * 10,
        out_specs=(in_vmem,) * 2,
        scratch_shapes=[
            pltpu.VMEM(kernel_hat.shape, BF16),
            pltpu.VMEM(coefficients.shape, F32),
            pltpu.VMEM(forward.shape[1:], F32),
            pltpu.VMEM(inverse.shape[1:], BF16),
            pltpu.VMEM((1, obs), jnp.int32),
            pltpu.VMEM((4, tall + 2 * EDGE, span), F32),
            pltpu.VMEM((tall + 2 * EDGE, wide), jnp.int32),
            pltpu.VMEM((tall + 2 * EDGE, span), F32),
            pltpu.VMEM((4, 4, EDGE, LANE), F32),
            pltpu.VMEM((4, EDGE, LANE), jnp.int32),
            pltpu.VMEM((32, tall), F32),
            pltpu.VMEM((32, tall), F32),
            pltpu.VMEM((n_cols, groups, 2 * GROUP, points), F32),
            pltpu.VMEM((n_cols - 1, groups, 2 * GROUP, points), F32),
            pltpu.VMEM((steps, points), F32),
            pltpu.VMEM((n_rows - 1, own_steps, points), F32),
            pltpu.VMEM((2, points), F32),
            pltpu.VMEM((n_cols - 1, n_rows, 2, points), F32),
            pltpu.VMEM((n_cols, 2, points), F32),
            pltpu.VMEM((3, tall + 2 * EDGE, span), F32),
            pltpu.VMEM((span, obs), BF16),
            dma((9,)),
            dma((groups, 2)),
            dma((14,)),
            dma((14,)),
            dma((groups, n_cols - 1)),
            dma((groups, n_cols - 1)),
            dma((n_rows - 1,)),
            dma((n_rows - 1,)),
            dma((n_cols - 1,)),
            dma((n_cols - 1, n_rows)),
        ],
        compiler_params=pltpu.CompilerParams(
            collective_id=0, has_side_effects=True, vmem_limit_bytes=60 * 1024 * 1024
        ),
    )(
        kernel_hat, coefficients, wave_speed_sq, wet_mask, boundary_cell.reshape(1, obs),
        height, flux_x, flux_y, jnp.asarray(forward), jnp.asarray(inverse),
    )
    return pl.pallas_call(
        write_out,
        out_shape=(
            jax.ShapeDtypeStruct((own_steps, points), F32),
            jax.ShapeDtypeStruct((tall, wide), F32),
            jax.ShapeDtypeStruct((tall, wide), F32),
            jax.ShapeDtypeStruct((tall, wide), F32),
        ),
        in_specs=[in_vmem] * 2,
        out_specs=(anywhere,) * 4,
        scratch_shapes=[dma((4,))],
        compiler_params=pltpu.CompilerParams(vmem_limit_bytes=4 * 1024 * 1024),
    )(series, fields)


def solution(mesh):
    n_rows, n_cols = mesh.shape["rows"], mesh.shape["cols"]
    return jax.shard_map(
        functools.partial(on_device, n_rows, n_cols),
        mesh=mesh,
        in_specs=(
            P(None, "rows", "cols", None),
            P(None, "cols"),
            P("rows", "cols"),
            P("rows", "cols"),
            P(),
            P("rows", "cols"),
            P("rows", "cols"),
            P("rows", "cols"),
        ),
        out_specs=(P("rows", "cols"), P("rows", "cols"), P("rows", "cols"), P("rows", "cols")),
        check_vma=False,
    )
```
